32 devices in a mesh: grp: 2 (over x), blk: 16 (over z, y, core).
Axes of the slice: x: 2, y: 2, z: 4, core: 2. Of those that a mesh axis runs over, the one named last changes fastest.
Arguments:
- atoms: bfloat16 [16384, 512], P(('grp', 'blk')), parts along dimension 0, may hold values from -8 to 8
- edge_mask: int32 [32, 5, 512, 512], P(('grp', 'blk')), parts along dimension 0, may hold values from 0 to 1
- norm_gain: float32 [512], replicated, may hold values from 0.25 to 1.75
- w_query: bfloat16 [512, 512], replicated, may hold values from -3 to 3
- w_key: bfloat16 [512, 512], replicated, may hold values from -3 to 3
- w_value: bfloat16 [512, 512], replicated, may hold values from -0.25 to 0.25
- w_out: bfloat16 [512, 512], replicated, may hold values from -0.25 to 0.25
- bn_gain: float32 [512], replicated, may hold values from 0.25 to 1.75
- bn_shift: float32 [512], replicated, may hold values from -3 to 3
- w_up: bfloat16 [512, 1024], replicated, may hold values from -0.25 to 0.25
- w_down: bfloat16 [1024, 512], replicated, may hold values from -0.1875 to 0.1875
Outputs:
- updated: bfloat16 [16384, 512], P(('grp', 'blk')), parts along dimension 0
The draws below stay inside these ranges and needn't reach their ends.
There are 2 independent parts, one for each index of `grp`. The reference program is written for one: setup_inputs(seed, part) draws one part's arguments, and reference() takes and returns one part's arrays. A program takes and returns all parts, laid end to end along the dimension named above; an argument that names none is the same for every part. Nothing has to cross between parts.
All inputs are finite; a program needn't handle non-finite values.
Results may differ from the reference program's by a relative error of at most 0.01.
The reference program's roundings to bfloat16 on the way (of `normed`, `query`, `weight`, `mixed`, `batched` and `hidden`) count: a program that leaves them out, or rounds other values in their place, can miss the bound.
Values may be sent and summed in bfloat16 or wider, within the bound.
A program may use at most 128 MiB of HBM per device.

```python
import jax
import jax.numpy as jnp
from jax import lax

D = 512
HEADS = 8
HEAD_DIM = 64
FF = 1024
REACH = 2
TILE = 512
ATOMS = 8192


def draw_atoms(key, part):
    key_base = jax.random.fold_in(key, 11)
    key_one, key_two, key_three, key_four = jax.random.split(key_base, 4)
    ntiles = ATOMS // TILE
    tile_ids = (jnp.arange(ATOMS) // TILE).astype(jnp.int32)
    tile_index = tile_ids.astype(jnp.float32)
    rising = (1.0 + 2.0 * tile_index / (ntiles - 1))[:, None]
    parity = (1 - 2 * (tile_ids % 2)).astype(jnp.float32)[:, None]
    row_scale = jnp.exp(jax.random.uniform(key_two, (ATOMS, 1), jnp.float32, -0.69, 0.69))
    noise = jnp.clip(jax.random.normal(key_one, (ATOMS, D), jnp.float32), -6.0, 6.0)
    feature_mean = jnp.clip(jax.random.normal(key_three, (1, D), jnp.float32), -3.0, 3.0)
    bulk = noise * row_scale * rising + feature_mean * rising
    alternate = jnp.clip(jax.random.normal(key_four, (1, D), jnp.float32), -3.0, 3.0)
    return (0.1 * (bulk + alternate * parity)).astype(jnp.bfloat16)


def projection_draw(key, salt):
    base = jax.random.normal(jax.random.fold_in(key, salt), (D, D), jnp.float32)
    base = jnp.clip(base, -4.0, 4.0) * D ** (-0.5)
    return base.astype(jnp.bfloat16)


def draw_w_query(key, part):
    return projection_draw(key, 21)


def draw_w_key(key, part):
    return projection_draw(key, 22)


def draw_edge_mask(key, part):
    ntiles = ATOMS // TILE
    widths = 2 * REACH + 1
    key_base = jax.random.fold_in(key, 31)
    key_one, key_two, key_three = jax.random.split(key_base, 3)
    cut_level = jax.random.randint(key_one, (ntiles, widths, 1, 1), 0, 12)
    own_level = jax.random.randint(key_two, (ntiles, widths, 1, 1), 6, 24)
    offset = jnp.arange(widths).reshape(1, widths, 1, 1)
    level = jnp.where(offset == REACH, own_level, cut_level)
    draws = jax.random.randint(key_three, (ntiles, widths, TILE, TILE), 0, 64)
    return (draws < level).astype(jnp.int32)


def centred(key, extent, scale, reach, dtype=jnp.bfloat16):
    values = scale * jax.random.normal(key, extent, jnp.float32)
    return jnp.clip(values, min=-reach, max=reach).astype(dtype)


def setup_inputs(seed: int = 0, part: int = 0) -> dict:
    splits = jax.random.split(jax.random.key(seed), 12)
    part_keys = jax.random.split(jax.random.fold_in(splits[11], part), 12)
    return {
        "atoms": draw_atoms(jax.random.fold_in(jax.random.fold_in(splits[11], part), 71), part),
        "edge_mask": draw_edge_mask(jax.random.fold_in(jax.random.fold_in(splits[11], part), 71), part),
        "norm_gain": jnp.clip(1.0 + 0.15 * jax.random.normal(splits[2], (D,), jnp.float32), 0.25, 1.75),
        "w_query": draw_w_query(jax.random.fold_in(splits[11], 71), part),
        "w_key": draw_w_key(jax.random.fold_in(splits[11], 71), part),
        "w_value": centred(splits[5], (D, D), D ** -0.5, 0.25),
        "w_out": centred(splits[6], (D, D), D ** -0.5, 0.25),
        "bn_gain": jnp.clip(1.0 + 0.15 * jax.random.normal(splits[7], (D,), jnp.float32), 0.25, 1.75),
        "bn_shift": centred(splits[8], (D,), 0.5, 3.0, jnp.float32),
        "w_up": centred(splits[9], (D, FF), D ** -0.5, 0.25),
        "w_down": centred(splits[10], (FF, D), FF ** -0.5, 0.1875),
    }


def reference(atoms, edge_mask, norm_gain, w_query, w_key, w_value, w_out, bn_gain, bn_shift, w_up, w_down):
    ntiles = ATOMS // TILE
    widths = 2 * REACH + 1
    scale = HEAD_DIM ** (-0.5)
    xfull = atoms.astype(jnp.float32)
    normed = (xfull * lax.rsqrt(lax.optimization_barrier(jnp.mean(xfull * xfull, axis=-1, keepdims=True)) + 1e-06) * norm_gain).astype(jnp.bfloat16)
    query = jnp.dot(normed, w_query, preferred_element_type=jnp.float32).astype(jnp.bfloat16)
    keys = jnp.dot(normed, w_key, preferred_element_type=jnp.float32).astype(jnp.bfloat16)
    values = jnp.dot(normed, w_value, preferred_element_type=jnp.float32).astype(jnp.bfloat16)
    q_tiles = query.reshape(ntiles, TILE, HEADS, HEAD_DIM)
    k_tiles = keys.reshape(ntiles, TILE, HEADS, HEAD_DIM)
    v_tiles = values.reshape(ntiles, TILE, HEADS, HEAD_DIM)
    k_near = jnp.stack([jnp.roll(k_tiles, -(o - REACH), axis=0) for o in range(widths)], axis=1).reshape(ntiles, widths * TILE, HEADS, HEAD_DIM)
    v_near = jnp.stack([jnp.roll(v_tiles, -(o - REACH), axis=0) for o in range(widths)], axis=1).reshape(ntiles, widths * TILE, HEADS, HEAD_DIM)
    rows = lax.broadcasted_iota(jnp.int32, (TILE, widths, TILE), 0)
    cols = lax.broadcasted_iota(jnp.int32, (TILE, widths, TILE), 2)
    block = lax.broadcasted_iota(jnp.int32, (TILE, widths, TILE), 1)
    selfmask = ((rows == cols) & (block == REACH)).reshape(TILE, widths * TILE)

    def one_tile(pieces):
        qpart, kpart, vpart, mpart = pieces
        allowed = (jnp.transpose(mpart, (1, 0, 2)).reshape(TILE, widths * TILE) > 0) | selfmask
        score = jnp.einsum('qhd,khd->hqk', qpart.astype(jnp.float32), kpart.astype(jnp.float32)) * scale
        score = jnp.where(allowed[None], score, -1e+30)
        top = lax.optimization_barrier(jnp.max(score, axis=-1, keepdims=True))
        expo = jnp.exp(score - top)
        total = lax.optimization_barrier(jnp.sum(expo, axis=-1))
        weight = expo.astype(jnp.bfloat16)
        summed = jnp.einsum('hqk,khd->qhd', weight.astype(jnp.float32), vpart.astype(jnp.float32))
        return (summed / jnp.transpose(total)[:, :, None]).reshape(TILE, D).astype(jnp.bfloat16)
    mixed = lax.map(one_tile, (q_tiles, k_near, v_near, edge_mask)).reshape(ATOMS, D)
    after = xfull + jnp.dot(mixed, w_out, preferred_element_type=jnp.float32)
    mean = lax.optimization_barrier(jnp.mean(after, axis=0))
    var = lax.optimization_barrier(jnp.mean((after - mean) ** 2, axis=0))
    batched = ((after - mean) * lax.rsqrt(var + 1e-05) * bn_gain + bn_shift).astype(jnp.bfloat16)
    hidden = jax.nn.gelu(jnp.dot(batched, w_up, preferred_element_type=jnp.float32), approximate=True).astype(jnp.bfloat16)
    return (after + jnp.dot(hidden, w_down, preferred_element_type=jnp.float32)).astype(jnp.bfloat16)
```

```python
import functools

import jax
import jax.numpy as jnp
from jax import lax
from jax.experimental import pallas as pl
from jax.experimental.pallas import tpu as pltpu
from jax.sharding import PartitionSpec as P

HEAD_DIM = 64
PAIR = 2 * HEAD_DIM
REACH = 2
CHUNKS = 4
NEG = -1e30
MESH = pl.DeviceIdType.MESH
PARTNER, MIRROR, RAIL, CROSS = 0, 1, 2, 3
ROWS_STEP = 256


def kernel(
    n,
    atoms_hbm, mask_hbm, ng_hbm, wq_hbm, wk_hbm, wv_hbm, wo_hbm, bg_hbm, bs_hbm, wu_hbm, wd_hbm,
    out_ref,
    x_ref, mask_ref, ng_ref, wq_ref, wk_ref, wv_ref, wo_ref, bg_ref, bs_ref, wu_ref, wd_ref,
    nb_ref, qm_ref, kb_ref, va_ref, bias_ref, m_ref, l_ref, acc_ref, mixed_ref, after_ref,
    stats_ref, load_sem, mask_sem,
    p_send, p_recv, m_send, m_recv, r_send, r_recv, c_send, c_recv, s_send, s_recv,
):
    me = lax.axis_index("blk")
    rows, width = x_ref.shape
    pairs = width // PAIR
    group, inside = me // 4, me % 4
    side, core = inside // 2, inside % 2
    partner = group * 4 + side * 2 + (1 - core)
    mirror = group * 4 + (1 - side) * 2 + core
    groups = n // 4
    rail_to = ((group + 1 - 2 * side + groups) % groups) * 4 + side * 2 + core
    cross_source = jnp.where(side == core, MIRROR, RAIL)

    barrier = pltpu.get_barrier_semaphore()

    def greet(d, carry):
        pl.semaphore_signal(
            barrier, inc=1, device_id={"blk": lax.rem(me + d, n)}, device_id_type=MESH
        )
        return carry

    lax.fori_loop(1, n, greet, 0)

    sources = (
        (atoms_hbm, x_ref), (ng_hbm, ng_ref), (wq_hbm, wq_ref), (wk_hbm, wk_ref), (wv_hbm, wv_ref),
        (wo_hbm, wo_ref), (bg_hbm, bg_ref), (bs_hbm, bs_ref), (wu_hbm, wu_ref), (wd_hbm, wd_ref),
    )
    loads = [
        pltpu.make_async_copy(src, dst, load_sem.at[i]) for i, (src, dst) in enumerate(sources)
    ]

    far = jnp.where(side == 0, 2, -2)
    near = jnp.where(core == 0, 1, -1)
    offsets = [jnp.int32(0), near, far, -far, -near]
    masks = [
        pltpu.make_async_copy(
            mask_hbm.at[0, offsets[i] + REACH], mask_ref.at[i], mask_sem.at[i]
        )
        for i in range(2 * REACH + 1)
    ]
    for i in range(5):
        loads[i].start()
    for mask_load in masks:
        mask_load.start()
    for i in range(5, len(loads)):
        loads[i].start()

    step_rows = rows // CHUNKS

    def chunk(c):
        return pl.ds(c * step_rows, step_rows)

    def mirror_copy(c):
        return pltpu.make_async_remote_copy(
            src_ref=x_ref.at[chunk(c)], dst_ref=nb_ref.at[MIRROR, chunk(c)],
            send_sem=m_send.at[c], recv_sem=m_recv.at[c],
            device_id={"blk": mirror}, device_id_type=MESH,
        )

    def rail_copy(c):
        return pltpu.make_async_remote_copy(
            src_ref=nb_ref.at[MIRROR, chunk(c)], dst_ref=nb_ref.at[RAIL, chunk(c)],
            send_sem=r_send.at[c], recv_sem=r_recv.at[c],
            device_id={"blk": rail_to}, device_id_type=MESH,
        )

    def cross_copy(c):
        return pltpu.make_async_remote_copy(
            src_ref=nb_ref.at[cross_source, chunk(c)], dst_ref=nb_ref.at[CROSS, chunk(c)],
            send_sem=c_send.at[c], recv_sem=c_recv.at[c],
            device_id={"blk": partner}, device_id_type=MESH,
        )

    partner_copy = pltpu.make_async_remote_copy(
        src_ref=x_ref, dst_ref=nb_ref.at[PARTNER], send_sem=p_send, recv_sem=p_recv,
        device_id={"blk": partner}, device_id_type=MESH,
    )

    def relay_rail(c):
        mirror_copy(c).wait_recv()
        rail_copy(c).start()

    def relay_cross(c):
        rail_copy(c).wait_recv()
        cross_copy(c).start()

    loads[0].wait()
    pl.semaphore_wait(barrier, n - 1)
    for c in range(CHUNKS):
        mirror_copy(c).start()
    partner_copy.start()

    def normalize(value):
        full = value.astype(jnp.float32)
        return (
            full * lax.rsqrt(jnp.mean(full * full, axis=-1, keepdims=True) + 1e-06) * ng_ref[...]
        ).astype(jnp.bfloat16)

    left = lax.broadcasted_iota(jnp.int32, (rows, PAIR), 1) < HEAD_DIM
    left_step = lax.broadcasted_iota(jnp.int32, (ROWS_STEP, PAIR), 1) < HEAD_DIM

    for h in range(pairs):
        va_ref[h, :, PAIR:] = jnp.ones((rows, PAIR), jnp.bfloat16)

    def set_keys(normed):
        keys = jnp.dot(normed, wk_ref[...], preferred_element_type=jnp.float32).astype(jnp.bfloat16)
        values = jnp.dot(normed, wv_ref[...], preferred_element_type=jnp.float32).astype(jnp.bfloat16)
        for h in range(pairs):
            kb_ref[h] = keys[:, h * PAIR:(h + 1) * PAIR]
            va_ref[h, :, :PAIR] = values[:, h * PAIR:(h + 1) * PAIR]

    def attend(i, first, between):
        masks[i].wait()
        allowed = mask_ref[i] > 0
        if i == 0:
            allowed = allowed | (
                lax.broadcasted_iota(jnp.int32, (rows, rows), 0)
                == lax.broadcasted_iota(jnp.int32, (rows, rows), 1)
            )
        bias_ref[...] = jnp.where(allowed, 0.0, NEG)

        def one_pair(h, carry):
            keys = kb_ref[h]
            values = va_ref[h]
            for r in range(0, rows, ROWS_STEP):
                piece = pl.ds(r, ROWS_STEP)
                results = []
                for j in range(2):
                    score = lax.dot_general(
                        qm_ref[2 * h + j, piece], keys, (((1,), (1,)), ((), ())),
                        preferred_element_type=jnp.float32,
                    ) + bias_ref[piece]
                    top = jnp.max(score, axis=-1, keepdims=True)
                    if first:
                        m_ref[2 * h + j, piece] = jnp.broadcast_to(top, (ROWS_STEP, PAIR))
                        factor = None
                    else:
                        old = m_ref[2 * h + j, piece]
                        new = jnp.maximum(old, top)
                        factor = jnp.exp(old - new)
                        m_ref[2 * h + j, piece] = new
                        top = new[:, :1]
                    weight = jnp.exp(score - top).astype(jnp.bfloat16)
                    product = jnp.dot(weight, values, preferred_element_type=jnp.float32)
                    results.append((factor, product))
                (fa, a), (fb, b) = results
                mixed = jnp.where(left_step, a[:, :PAIR], b[:, :PAIR])
                total = jnp.where(left_step, a[:, PAIR:], b[:, PAIR:])
                if first:
                    acc_ref[h, piece] = mixed
                    l_ref[h, piece] = total
                else:
                    factor = jnp.where(left_step, fa, fb)
                    acc_ref[h, piece] = acc_ref[h, piece] * factor + mixed
                    l_ref[h, piece] = l_ref[h, piece] * factor + total
            between(h)
            return carry

        lax.fori_loop(0, pairs, one_pair, 0)

    def at_odd(relay, base):
        def run(h):
            @pl.when(lax.rem(h, 2) == 1)
            def _():
                relay(base + h // 2)
        return run

    def nothing(h):
        pass

    loads[1].wait()
    normed = normalize(x_ref[...])
    loads[2].wait()
    query = jnp.dot(normed, wq_ref[...], preferred_element_type=jnp.float32).astype(jnp.bfloat16)
    query = query * jnp.bfloat16(HEAD_DIM ** (-0.5))
    zero = jnp.zeros((rows, PAIR), jnp.bfloat16)
    for h in range(pairs):
        piece = query[:, h * PAIR:(h + 1) * PAIR]
        qm_ref[2 * h] = jnp.where(left, piece, zero)
        qm_ref[2 * h + 1] = jnp.where(left, zero, piece)
    loads[3].wait()
    loads[4].wait()
    set_keys(normed)
    attend(0, True, at_odd(relay_rail, 0))

    partner_copy.wait_recv()
    set_keys(normalize(nb_ref[PARTNER]))
    attend(1, False, at_odd(relay_rail, 2))

    set_keys(normalize(nb_ref[MIRROR]))
    attend(2, False, at_odd(relay_cross, 0))

    for c in range(CHUNKS // 2, CHUNKS):
        relay_cross(c)
    set_keys(normalize(nb_ref[RAIL]))
    attend(3, False, nothing)

    for c in range(CHUNKS):
        cross_copy(c).wait_recv()
    set_keys(normalize(nb_ref[CROSS]))
    attend(4, False, nothing)

    for h in range(pairs):
        mixed_ref[:, h * PAIR:(h + 1) * PAIR] = (acc_ref[h] / l_ref[h]).astype(jnp.bfloat16)
    for load in loads[5:]:
        load.wait()
    after_ref[...] = x_ref[...].astype(jnp.float32) + jnp.dot(
        mixed_ref[...], wo_ref[...], preferred_element_type=jnp.float32
    )

    local_mean = jnp.sum(after_ref[...], axis=0, keepdims=True) * (1.0 / rows)
    spread = after_ref[...] - local_mean
    stats_ref[0, 0:1] = local_mean
    stats_ref[0, 1:2] = jnp.sum(spread * spread, axis=0, keepdims=True)

    def stats_copy(d):
        return pltpu.make_async_remote_copy(
            src_ref=stats_ref.at[0], dst_ref=stats_ref.at[d],
            send_sem=s_send.at[d], recv_sem=s_recv.at[d],
            device_id={"blk": lax.rem(me + d, n)}, device_id_type=MESH,
        )

    def send_stats(d, carry):
        stats_copy(d).start()
        return carry

    def take_stats(d, carry):
        stats_copy(d).wait_recv()
        return carry

    lax.fori_loop(1, n, send_stats, 0)

    partner_copy.wait_send()
    for c in range(CHUNKS):
        mirror_copy(c).wait_send()
        rail_copy(c).wait_send()
        cross_copy(c).wait_send()

    lax.fori_loop(1, n, take_stats, 0)
    gathered = stats_ref[...]
    means = gathered[:, 0, :]
    mean = jnp.sum(means, axis=0, keepdims=True) * (1.0 / n)
    shifts = means - mean
    var = (
        jnp.sum(gathered[:, 1, :], axis=0, keepdims=True) * (1.0 / rows)
        + jnp.sum(shifts * shifts, axis=0, keepdims=True)
    ) * (1.0 / n)
    gain = lax.rsqrt(var + 1e-05) * bg_ref[...]
    batched = ((after_ref[...] - mean) * gain + bs_ref[...]).astype(jnp.bfloat16)
    hidden = jax.nn.gelu(
        jnp.dot(batched, wu_ref[...], preferred_element_type=jnp.float32), approximate=True
    ).astype(jnp.bfloat16)
    out_ref[...] = (
        after_ref[...] + jnp.dot(hidden, wd_ref[...], preferred_element_type=jnp.float32)
    ).astype(jnp.bfloat16)

    def sent_stats(d, carry):
        stats_copy(d).wait_send()
        return carry

    lax.fori_loop(1, n, sent_stats, 0)


def body(
    atoms, edge_mask, norm_gain, w_query, w_key, w_value, w_out, bn_gain, bn_shift, w_up, w_down
):
    n = lax.axis_size("blk")
    rows, width = atoms.shape
    ff = w_up.shape[1]
    slabs = edge_mask.shape[1]
    pairs = width // PAIR
    bf16, f32 = jnp.bfloat16, jnp.float32
    dma = pltpu.SemaphoreType.DMA
    return pl.pallas_call(
        functools.partial(kernel, n),
        out_shape=jax.ShapeDtypeStruct((rows, width), bf16),
        in_specs=[pl.BlockSpec(memory_space=pl.ANY)] * 11,
        out_specs=pl.BlockSpec(memory_space=pltpu.VMEM),
        scratch_shapes=[
            pltpu.VMEM((rows, width), bf16),
            pltpu.VMEM((slabs, rows, rows), jnp.int32),
            pltpu.VMEM((1, width), f32),
            pltpu.VMEM((width, width), bf16),
            pltpu.VMEM((width, width), bf16),
            pltpu.VMEM((width, width), bf16),
            pltpu.VMEM((width, width), bf16),
            pltpu.VMEM((1, width), f32),
            pltpu.VMEM((1, width), f32),
            pltpu.VMEM((width, ff), bf16),
            pltpu.VMEM((ff, width), bf16),
            pltpu.VMEM((4, rows, width), bf16),
            pltpu.VMEM((2 * pairs, rows, PAIR), bf16),
            pltpu.VMEM((pairs, rows, PAIR), bf16),
            pltpu.VMEM((pairs, rows, 2 * PAIR), bf16),
            pltpu.VMEM((rows, rows), f32),
            pltpu.VMEM((2 * pairs, rows, PAIR), f32),
            pltpu.VMEM((pairs, rows, PAIR), f32),
            pltpu.VMEM((pairs, rows, PAIR), f32),
            pltpu.VMEM((rows, width), bf16),
            pltpu.VMEM((rows, width), f32),
            pltpu.VMEM((n, 2, width), f32),
            dma((10,)),
            dma((slabs,)),
            dma, dma,
            dma((CHUNKS,)), dma((CHUNKS,)),
            dma((CHUNKS,)), dma((CHUNKS,)),
            dma((CHUNKS,)), dma((CHUNKS,)),
            dma((n,)), dma((n,)),
        ],
        compiler_params=pltpu.CompilerParams(
            collective_id=0, has_side_effects=True, vmem_limit_bytes=60 * 1024 * 1024
        ),
    )(
        atoms, edge_mask, norm_gain.reshape(1, width), w_query, w_key, w_value, w_out,
        bn_gain.reshape(1, width), bn_shift.reshape(1, width), w_up, w_down,
    )


def solution(mesh):
    placed = (
        P(("grp", "blk"), None),
        P(("grp", "blk"), None, None, None),
        P(), P(), P(), P(), P(), P(), P(), P(), P(),
    )
    return jax.shard_map(
        body, mesh=mesh, in_specs=placed, out_specs=P(("grp", "blk"), None), check_vma=False
    )
```

```python
import functools

import jax
import jax.numpy as jnp
from jax import lax
from jax.experimental import pallas as pl
from jax.experimental.pallas import tpu as pltpu
from jax.sharding import PartitionSpec as P

HEAD_DIM = 64
PAIR = 2 * HEAD_DIM
REACH = 2
CHUNKS = 4
NEG = -1e30
MESH = pl.DeviceIdType.MESH
PARTNER, MIRROR, RAIL, CROSS = 0, 1, 2, 3
ROWS_STEP = 128
UNROLL = 2
SLOTS = 2


def kernel(
    n,
    atoms_hbm, mask_hbm, ng_hbm, wq_hbm, wk_hbm, wv_hbm, wo_hbm, bg_hbm, bs_hbm, wu_hbm, wd_hbm,
    out_ref,
    x_ref, mask_ref, ng_ref, wq_ref, wk_ref, wv_ref, wo_ref, bg_ref, bs_ref, wu_ref, wd_ref,
    nb_ref, qm_ref, kb_ref, va_ref, bias_ref, m_ref, l_ref, acc_ref, mixed_ref, after_ref,
    stats_ref, load_sem, mask_sem,
    p_send, p_recv, m_send, m_recv, r_send, r_recv, c_send, c_recv, s_send, s_recv,
):
    me = lax.axis_index("blk")
    rows, width = x_ref.shape
    pairs = width // PAIR
    group, inside = me // 4, me % 4
    side, core = inside // 2, inside % 2
    partner = group * 4 + side * 2 + (1 - core)
    mirror = group * 4 + (1 - side) * 2 + core
    groups = n // 4
    rail_to = ((group + 1 - 2 * side + groups) % groups) * 4 + side * 2 + core
    cross_source = jnp.where(side == core, MIRROR, RAIL)

    barrier = pltpu.get_barrier_semaphore()

    def greet(d, carry):
        pl.semaphore_signal(
            barrier, inc=1, device_id={"blk": lax.rem(me + d, n)}, device_id_type=MESH
        )
        return carry

    lax.fori_loop(1, n, greet, 0)

    sources = (
        (atoms_hbm, x_ref), (ng_hbm, ng_ref), (wq_hbm, wq_ref), (wk_hbm, wk_ref), (wv_hbm, wv_ref),
        (wo_hbm, wo_ref), (bg_hbm, bg_ref), (bs_hbm, bs_ref), (wu_hbm, wu_ref), (wd_hbm, wd_ref),
    )
    loads = [
        pltpu.make_async_copy(src, dst, load_sem.at[i]) for i, (src, dst) in enumerate(sources)
    ]

    far = jnp.where(side == 0, 2, -2)
    near = jnp.where(core == 0, 1, -1)
    offsets = [jnp.int32(0), near, far, -far, -near]
    masks = [
        pltpu.make_async_copy(
            mask_hbm.at[0, offsets[i] + REACH], mask_ref.at[i], mask_sem.at[i]
        )
        for i in range(2 * REACH + 1)
    ]
    for i in range(5):
        loads[i].start()
    for mask_load in masks:
        mask_load.start()
    for i in range(5, len(loads)):
        loads[i].start()

    step_rows = rows // CHUNKS

    def chunk(c):
        return pl.ds(c * step_rows, step_rows)

    def mirror_copy(c):
        return pltpu.make_async_remote_copy(
            src_ref=x_ref.at[chunk(c)], dst_ref=nb_ref.at[MIRROR, chunk(c)],
            send_sem=m_send.at[c], recv_sem=m_recv.at[c],
            device_id={"blk": mirror}, device_id_type=MESH,
        )

    def rail_copy(c):
        return pltpu.make_async_remote_copy(
            src_ref=nb_ref.at[MIRROR, chunk(c)], dst_ref=nb_ref.at[RAIL, chunk(c)],
            send_sem=r_send.at[c], recv_sem=r_recv.at[c],
            device_id={"blk": rail_to}, device_id_type=MESH,
        )

    def cross_copy(c):
        return pltpu.make_async_remote_copy(
            src_ref=nb_ref.at[cross_source, chunk(c)], dst_ref=nb_ref.at[CROSS, chunk(c)],
            send_sem=c_send.at[c], recv_sem=c_recv.at[c],
            device_id={"blk": partner}, device_id_type=MESH,
        )

    partner_copy = pltpu.make_async_remote_copy(
        src_ref=x_ref, dst_ref=nb_ref.at[PARTNER], send_sem=p_send, recv_sem=p_recv,
        device_id={"blk": partner}, device_id_type=MESH,
    )

    def relay_rail(c):
        mirror_copy(c).wait_recv()
        rail_copy(c).start()

    def relay_cross(c):
        rail_copy(c).wait_recv()
        cross_copy(c).start()

    def normalize(value):
        full = value.astype(jnp.float32)
        return (
            full * lax.rsqrt(jnp.mean(full * full, axis=-1, keepdims=True) + 1e-06) * ng_ref[...]
        ).astype(jnp.bfloat16)

    left = lax.broadcasted_iota(jnp.int32, (rows, PAIR), 1) < HEAD_DIM
    left_step = lax.broadcasted_iota(jnp.int32, (ROWS_STEP, PAIR), 1) < HEAD_DIM
    pieces = rows // ROWS_STEP

    for g in range(SLOTS):
        for h in range(pairs):
            va_ref[g, h, :, PAIR:] = jnp.ones((rows, PAIR), jnp.bfloat16)

    def set_keys(g, normed):
        keys = jnp.dot(normed, wk_ref[...], preferred_element_type=jnp.float32).astype(jnp.bfloat16)
        values = jnp.dot(normed, wv_ref[...], preferred_element_type=jnp.float32).astype(jnp.bfloat16)
        for h in range(pairs):
            kb_ref[g, h] = keys[:, h * PAIR:(h + 1) * PAIR]
            va_ref[g, h, :, :PAIR] = values[:, h * PAIR:(h + 1) * PAIR]

    def set_bias(g, i):
        masks[i].wait()
        allowed = mask_ref[i] > 0
        if i == 0:
            allowed = allowed | (
                lax.broadcasted_iota(jnp.int32, (rows, rows), 0)
                == lax.broadcasted_iota(jnp.int32, (rows, rows), 1)
            )
        bias_ref[g] = jnp.where(allowed, 0.0, NEG)

    def attend(count, first, between):
        blocks = rows // PAIR

        def scores(h, r):
            piece = pl.ds(r * ROWS_STEP, ROWS_STEP)
            found = []
            peaks = [None, None]
            for g in range(count):
                score = lax.dot_general(
                    qm_ref[h, r], kb_ref[g, h], (((1,), (1,)), ((), ())),
                    preferred_element_type=jnp.float32,
                )
                for b in range(blocks):
                    bias = bias_ref[g, piece, b * PAIR:(b + 1) * PAIR]
                    both = []
                    for j in range(2):
                        part = score[
                            j * ROWS_STEP:(j + 1) * ROWS_STEP, b * PAIR:(b + 1) * PAIR
                        ] + bias
                        peaks[j] = part if peaks[j] is None else jnp.maximum(peaks[j], part)
                        both.append(part)
                    found.append(both)
            return found, peaks

        def finish(h, r, found, peaks):
            piece = pl.ds(r * ROWS_STEP, ROWS_STEP)
            if not first:
                old = m_ref[h, piece]
                peaks = [
                    jnp.maximum(peaks[0], jnp.where(left_step, old, NEG)),
                    jnp.maximum(peaks[1], jnp.where(left_step, NEG, old)),
                ]
            tops = [
                jnp.broadcast_to(jnp.max(peak, axis=-1, keepdims=True), (ROWS_STEP, PAIR))
                for peak in peaks
            ]
            new = jnp.where(left_step, tops[0], tops[1])
            m_ref[h, piece] = new
            result = None
            for g in range(count):
                weight = jnp.concatenate([
                    jnp.concatenate([
                        jnp.exp(found[g * blocks + b][j] - tops[j]).astype(jnp.bfloat16)
                        for b in range(blocks)
                    ], axis=1)
                    for j in range(2)
                ], axis=0)
                product = jnp.dot(weight, va_ref[g, h], preferred_element_type=jnp.float32)
                result = product if result is None else result + product
            mixed = jnp.where(left_step, result[:ROWS_STEP, :PAIR], result[ROWS_STEP:, :PAIR])
            total = jnp.where(left_step, result[:ROWS_STEP, PAIR:], result[ROWS_STEP:, PAIR:])
            if first:
                acc_ref[h, piece] = mixed
                l_ref[h, piece] = total
            else:
                factor = jnp.exp(old - new)
                acc_ref[h, piece] = acc_ref[h, piece] * factor + mixed
                l_ref[h, piece] = l_ref[h, piece] * factor + total

        def some_pairs(t, carry):
            units = [(t * UNROLL + u, r) for u in range(UNROLL) for r in range(pieces)]
            ahead = scores(*units[0])
            for k, unit in enumerate(units):
                current = ahead
                if k + 1 < len(units):
                    ahead = scores(*units[k + 1])
                finish(*unit, *current)
            between(t)
            return carry

        lax.fori_loop(0, pairs // UNROLL, some_pairs, 0)

    half = CHUNKS // 2

    def each(relay, base):
        def run(t):
            for u in range(UNROLL):
                h = t * UNROLL + u
                @pl.when(lax.rem(h, 2) == 1)
                def _():
                    relay(base + h // 2)
        return run

    def nothing(t):
        pass

    loads[0].wait()
    loads[1].wait()
    normed = normalize(x_ref[...])
    loads[2].wait()
    query = jnp.dot(normed, wq_ref[...], preferred_element_type=jnp.float32).astype(jnp.bfloat16)
    query = query * jnp.bfloat16(HEAD_DIM ** (-0.5))
    zero = jnp.zeros((rows, PAIR), jnp.bfloat16)
    for h in range(pairs):
        piece = query[:, h * PAIR:(h + 1) * PAIR]
        first_head = jnp.where(left, piece, zero)
        second_head = jnp.where(left, zero, piece)
        for r in range(pieces):
            qm_ref[h, r, :ROWS_STEP] = first_head[r * ROWS_STEP:(r + 1) * ROWS_STEP]
            qm_ref[h, r, ROWS_STEP:] = second_head[r * ROWS_STEP:(r + 1) * ROWS_STEP]
    loads[3].wait()
    loads[4].wait()
    set_keys(0, normed)
    pl.semaphore_wait(barrier, n - 1)
    partner_copy.start()
    for c in range(CHUNKS):
        mirror_copy(c).start()
    set_bias(0, 0)
    attend(1, True, each(relay_rail, 0))

    partner_copy.wait_recv()
    set_keys(0, normalize(nb_ref[PARTNER]))
    set_bias(0, 1)
    attend(1, False, each(relay_rail, half))

    set_keys(0, normalize(nb_ref[MIRROR]))
    set_bias(0, 2)
    attend(1, False, each(relay_cross, 0))

    for c in range(half, CHUNKS):
        relay_cross(c)
    set_keys(0, normalize(nb_ref[RAIL]))
    set_bias(0, 3)
    for c in range(CHUNKS):
        cross_copy(c).wait_recv()
    set_keys(1, normalize(nb_ref[CROSS]))
    set_bias(1, 4)
    attend(2, False, nothing)

    for h in range(pairs):
        mixed_ref[:, h * PAIR:(h + 1) * PAIR] = (acc_ref[h] / l_ref[h]).astype(jnp.bfloat16)
    for load in loads[5:]:
        load.wait()
    after_ref[...] = x_ref[...].astype(jnp.float32) + jnp.dot(
        mixed_ref[...], wo_ref[...], preferred_element_type=jnp.float32
    )

    local_mean = jnp.sum(after_ref[...], axis=0, keepdims=True) * (1.0 / rows)
    spread = after_ref[...] - local_mean
    stats_ref[0, 0:1] = local_mean
    stats_ref[0, 1:2] = jnp.sum(spread * spread, axis=0, keepdims=True)

    def stats_copy(d):
        return pltpu.make_async_remote_copy(
            src_ref=stats_ref.at[0], dst_ref=stats_ref.at[d],
            send_sem=s_send.at[d], recv_sem=s_recv.at[d],
            device_id={"blk": lax.rem(me + d, n)}, device_id_type=MESH,
        )

    def send_stats(d, carry):
        stats_copy(d).start()
        return carry

    def take_stats(d, carry):
        stats_copy(d).wait_recv()
        return carry

    lax.fori_loop(1, n, send_stats, 0)

    partner_copy.wait_send()
    for c in range(CHUNKS):
        mirror_copy(c).wait_send()
        rail_copy(c).wait_send()
        cross_copy(c).wait_send()

    lax.fori_loop(1, n, take_stats, 0)
    gathered = stats_ref[...]
    means = gathered[:, 0, :]
    mean = jnp.sum(means, axis=0, keepdims=True) * (1.0 / n)
    shifts = means - mean
    var = (
        jnp.sum(gathered[:, 1, :], axis=0, keepdims=True) * (1.0 / rows)
        + jnp.sum(shifts * shifts, axis=0, keepdims=True)
    ) * (1.0 / n)
    gain = lax.rsqrt(var + 1e-05) * bg_ref[...]
    batched = ((after_ref[...] - mean) * gain + bs_ref[...]).astype(jnp.bfloat16)
    hidden = jax.nn.gelu(
        jnp.dot(batched, wu_ref[...], preferred_element_type=jnp.float32), approximate=True
    ).astype(jnp.bfloat16)
    out_ref[...] = (
        after_ref[...] + jnp.dot(hidden, wd_ref[...], preferred_element_type=jnp.float32)
    ).astype(jnp.bfloat16)

    def sent_stats(d, carry):
        stats_copy(d).wait_send()
        return carry

    lax.fori_loop(1, n, sent_stats, 0)


def body(
    atoms, edge_mask, norm_gain, w_query, w_key, w_value, w_out, bn_gain, bn_shift, w_up, w_down
):
    n = lax.axis_size("blk")
    rows, width = atoms.shape
    ff = w_up.shape[1]
    slabs = edge_mask.shape[1]
    pairs = width // PAIR
    bf16, f32 = jnp.bfloat16, jnp.float32
    dma = pltpu.SemaphoreType.DMA
    return pl.pallas_call(
        functools.partial(kernel, n),
        out_shape=jax.ShapeDtypeStruct((rows, width), bf16),
        in_specs=[pl.BlockSpec(memory_space=pl.ANY)] * 11,
        out_specs=pl.BlockSpec(memory_space=pltpu.VMEM),
        scratch_shapes=[
            pltpu.VMEM((rows, width), bf16),
            pltpu.VMEM((slabs, rows, rows), jnp.int32),
            pltpu.VMEM((1, width), f32),
            pltpu.VMEM((width, width), bf16),
            pltpu.VMEM((width, width), bf16),
            pltpu.VMEM((width, width), bf16),
            pltpu.VMEM((width, width), bf16),
            pltpu.VMEM((1, width), f32),
            pltpu.VMEM((1, width), f32),
            pltpu.VMEM((width, ff), bf16),
            pltpu.VMEM((ff, width), bf16),
            pltpu.VMEM((4, rows, width), bf16),
            pltpu.VMEM((pairs, rows // ROWS_STEP, 2 * ROWS_STEP, PAIR), bf16),
            pltpu.VMEM((SLOTS, pairs, rows, PAIR), bf16),
            pltpu.VMEM((SLOTS, pairs, rows, 2 * PAIR), bf16),
            pltpu.VMEM((SLOTS, rows, rows), f32),
            pltpu.VMEM((pairs, rows, PAIR), f32),
            pltpu.VMEM((pairs, rows, PAIR), f32),
            pltpu.VMEM((pairs, rows, PAIR), f32),
            pltpu.VMEM((rows, width), bf16),
            pltpu.VMEM((rows, width), f32),
            pltpu.VMEM((n, 2, width), f32),
            dma((10,)),
            dma((slabs,)),
            dma, dma,
            dma((CHUNKS,)), dma((CHUNKS,)),
            dma((CHUNKS,)), dma((CHUNKS,)),
            dma((CHUNKS,)), dma((CHUNKS,)),
            dma((n,)), dma((n,)),
        ],
        compiler_params=pltpu.CompilerParams(
            collective_id=0, has_side_effects=True, vmem_limit_bytes=60 * 1024 * 1024
        ),
    )(
        atoms, edge_mask, norm_gain.reshape(1, width), w_query, w_key, w_value, w_out,
        bn_gain.reshape(1, width), bn_shift.reshape(1, width), w_up, w_down,
    )


def solution(mesh):
    placed = (
        P(("grp", "blk"), None),
        P(("grp", "blk"), None, None, None),
        P(), P(), P(), P(), P(), P(), P(), P(), P(),
    )
    return jax.shard_map(
        body, mesh=mesh, in_specs=placed, out_specs=P(("grp", "blk"), None), check_vma=False
    )
```
